32 devices in a mesh: dp: 8 (over z, y), expert: 4 (over x, core).
Axes of the slice: x: 2, y: 2, z: 4, core: 2. Of those that a mesh axis runs over, the one named last changes fastest.
Arguments:
- queries: bfloat16 [4096, 4096], P('dp', 'expert'), may hold values from -6 to 6
- key_states: bfloat16 [4096, 4096], P('dp', 'expert'), may hold values from -6 to 6
- value_states: bfloat16 [4096, 4096], P('dp', 'expert'), may hold values from -6 to 6
- doc_lengths: int32 [8, 8], replicated, may hold values from 0 to 512, as said below
- move_plan: int32 [8, 2], replicated, may hold values from 0 to 7, as said below
- expert_ids: int32 [4096, 8], P('dp'), may hold values from 0 to 15, all different within a row; in each aligned block of 512 rows (0 to 511, 512 to 1023, ...) at most 384 rows name the same one
- gate_weights: float32 [4096, 8], P('dp'), may hold values from 0.05 to 0.5
- expert_weight: bfloat16 [16, 4096, 1024], P('expert'), may hold values from -0.29882812 to 0.29882812
Outputs:
- attended: bfloat16 [4096, 4096], P('dp', 'expert')
- combined: bfloat16 [4096, 1024], P('dp', 'expert')
- row_load: float32 [8], P('dp')
The draws below stay inside these ranges and needn't reach their ends.
Inputs may be any that keep to these rules, and one draw needn't show every extreme that they name: `doc_lengths`: each row's entries are the lengths of its packed documents in order and sum to 512; a zero marks an absent document; some row holds a single document. move_plan[r, 0] is r itself or the row half the dp axis away, (r + 8 / 2) mod 8; a row is handed to its partner only if its pairs in all exceed the partner's, so two partners never both move; move_plan[r, 1] is a block number below 2; at least one row moves a block. `expert_ids`: each token names 8 different experts; among the 512 tokens of one row no expert is named by more than 384 tokens.
All inputs are finite; a program needn't handle non-finite values.
Results may differ from the reference program's by a relative error of at most 0.0095.
Values may be sent and summed in bfloat16 or wider, within the bound.
A program may use at most 128 MiB of HBM per device.

```python
import math
import jax
import jax.numpy as jnp
import numpy as np
from jax import lax

HEADS = 32
HEAD_DIM = 128
QBLOCK = 128
BLOCKS = 4
MAX_DOCS = 8
EXPERT_FF = 1024
EXPERTS = 16
TOPK = 8
ROW_TOKENS = 512
TOKENS = 4096
D_ATT = 4096
CAP = 384
N_DP = 8


def joint_states(key):
    first = jax.random.normal(jax.random.fold_in(key, 11), (TOKENS, D_ATT), jnp.float32)
    second = jax.random.normal(jax.random.fold_in(key, 12), (TOKENS, D_ATT), jnp.float32)
    first = jnp.clip(first, -6.0, 6.0)
    second = jnp.clip(second, -6.0, 6.0)
    return (first, second)


def draw_queries(key, part):
    return joint_states(key)[0].astype(jnp.bfloat16)


def draw_key_states(key, part):
    return joint_states(key)[1].astype(jnp.bfloat16)


def lengths_table(key):
    row_ids = jnp.arange(N_DP, dtype=jnp.int32)
    counts = jax.random.randint(jax.random.fold_in(key, 21), (N_DP, 1), 1, MAX_DOCS + 1)
    single = jax.random.randint(jax.random.fold_in(key, 22), (), 0, N_DP)
    counts = jnp.where(row_ids[:, None] == single, 1, counts)
    raw_cuts = jax.random.randint(jax.random.fold_in(key, 23), (N_DP, MAX_DOCS - 1), 1, ROW_TOKENS)
    used = jnp.arange(MAX_DOCS - 1, dtype=jnp.int32)[None, :] < counts - 1
    cuts = jnp.sort(jnp.where(used, raw_cuts, ROW_TOKENS), axis=1)
    edges = jnp.concatenate([jnp.zeros((N_DP, 1), jnp.int32), cuts.astype(jnp.int32), jnp.full((N_DP, 1), ROW_TOKENS, jnp.int32)], 1)
    return (edges[:, 1:] - edges[:, :-1]).astype(jnp.int32)


def draw_doc_lengths(key, part):
    return lengths_table(key)


def draw_move_plan(key, part):
    lengths = lengths_table(key)
    bounds = jnp.cumsum(lengths, axis=1).astype(jnp.int32)
    positions = jnp.arange(ROW_TOKENS, dtype=jnp.int32)
    starts = jnp.max(jnp.where(bounds[:, None, :] <= positions[None, :, None], bounds[:, None, :], 0), axis=2)
    pairs = (positions[None, :] - starts + 1).reshape(N_DP, BLOCKS, QBLOCK).sum(axis=2)
    totals = jnp.sum(pairs, axis=1)
    row_ids = jnp.arange(N_DP, dtype=jnp.int32)
    partner = (row_ids + N_DP // 2) % N_DP
    moves = totals > totals[partner]
    heavy = jnp.argmax(totals).astype(jnp.int32)
    moves = jnp.where(jnp.any(moves), moves, row_ids == heavy)
    blocks = jnp.argmax(pairs[:, :BLOCKS // 2], axis=1).astype(jnp.int32)
    runner = jnp.where(moves, partner, row_ids)
    return jnp.stack([runner, blocks], 1).astype(jnp.int32)


def shard_levels(own_key, extent, cuts, smallest, largest):
    gain = 1.0
    for axis_at, parts in cuts:
        steps = jax.random.uniform(jax.random.fold_in(jax.random.fold_in(own_key, 6), axis_at), (parts,), jnp.float32, smallest / len(cuts), largest / len(cuts))
        gain = gain * jnp.repeat(jnp.exp(steps), extent[axis_at] // parts).reshape((-1,) + (1,) * (len(extent) - 1 - axis_at))
    return gain


def routed_block(stream_key, own, number, rows, count, top, reach, slope):
    ranking = jax.random.permutation(stream_key, count)
    crowded, usual = portions_of(count, rows * top, reach, slope, True), portions_of(count, rows * top, reach, slope, False)
    places = jnp.arange(count)

    def named(tallies, offset_by):
        used = int((tallies > 0).sum())
        fixed = max(1, used // 4)
        passed = fixed + (places - fixed + offset_by * (used - fixed)) % max(1, count - fixed)
        return jnp.zeros((count,), jnp.int32).at[ranking[jnp.where(places < fixed, places, passed)]].set(jnp.asarray(tallies, jnp.int32))

    tallies = jnp.where(number % 4 == 0, named(crowded, number // 4), named(usual, number - number // 4 - 1))
    mixed = jax.random.permutation(jax.random.fold_in(own, 3), count)
    source_of, receiver = mixed[0:count // 2 * 2:2], mixed[1:count // 2 * 2:2]
    slack = jnp.minimum(tallies[source_of] - 1, reach - tallies[receiver]) // 2
    slack = jnp.where((source_of == ranking[0]) | (receiver == ranking[0]) | (tallies[receiver] == 0), 0, jnp.maximum(slack, 0))
    passed = jax.random.randint(jax.random.fold_in(own, 4), (count // 2,), 0, 1 << 20) % (slack + 1)
    tallies = tallies.at[source_of].add(-passed).at[receiver].add(passed)
    labels = jnp.searchsorted(jnp.cumsum(tallies), jnp.arange(rows * top), side="right").astype(jnp.int32)
    listing = labels.reshape(top, rows).T
    listing = listing[jax.random.permutation(jax.random.fold_in(own, 1), rows)]
    offset_by = jax.random.randint(jax.random.fold_in(own, 2), (rows, 1), 0, top)
    return jnp.take_along_axis(listing, (jnp.arange(top)[None, :] + offset_by) % top, axis=1)


def portions_of(count, total, most, skew, full):
    weights = [(1 << 20) // math.isqrt(grade ** skew) + 1 for grade in range(1, count + 1)]
    largest = most if full else min(most, max(-(-total // count), total * weights[0] // sum(weights)))
    least = 1 if total - largest >= count - 1 else 0
    given, rest = [largest] + [least] * (count - 1), total - largest - least * (count - 1)
    while rest > 0:
        movable = [i for i in range(1, count) if given[i] < largest] or [i for i in range(1, count) if given[i] < most]
        pool, remaining = sum([weights[i] for i in movable]), rest
        for i in movable:
            more = min(most - given[i], max(1, remaining * weights[i] // pool), rest)
            given[i] = given[i] + more
            rest = rest - more
    return np.array(given)


def scatter_about(stream_key, extent, scale, most, cuts=(), kind=jnp.bfloat16):
    entries = jax.random.normal(stream_key, extent, jnp.float32) * scale
    if len(cuts) > 0:
        entries = shard_levels(stream_key, extent, cuts, -0.22, 0.18) * entries
    return jnp.clip(entries, min=-most, max=most).astype(kind)


def setup_inputs(seed: int = 0) -> dict:
    streams_of = jax.random.split(jax.random.key(seed), 9)
    queries = draw_queries(jax.random.fold_in(streams_of[8], 71), 0)
    key_states = draw_key_states(jax.random.fold_in(streams_of[8], 71), 0)
    value_states = scatter_about(streams_of[2], (TOKENS, D_ATT), 1.0, 6.0, ((0, 8), (1, 4)))
    doc_lengths = draw_doc_lengths(jax.random.fold_in(streams_of[8], 71), 0)
    move_plan = draw_move_plan(jax.random.fold_in(streams_of[8], 71), 0)
    expert_ids_keys = jax.random.split(jax.random.fold_in(streams_of[5], 1), TOKENS // ROW_TOKENS)
    expert_ids_turns = jax.random.permutation(jax.random.fold_in(streams_of[5], 3), TOKENS // ROW_TOKENS)
    expert_ids = jax.vmap(lambda own, number: routed_block(jax.random.fold_in(streams_of[5], 2), own, number, ROW_TOKENS, EXPERTS, TOPK, CAP, 1))(expert_ids_keys, expert_ids_turns).reshape((TOKENS, TOPK))
    gate_weights = jnp.clip(0.05 + 0.45 * jax.random.uniform(streams_of[6], (TOKENS, TOPK), jnp.float32) ** shard_levels(streams_of[6], (TOKENS, TOPK), ((0, 8),), -0.2, 0.2), 0.05, 0.5)
    expert_weight = scatter_about(streams_of[7], (EXPERTS, D_ATT, EXPERT_FF), 0.05, 0.29882812, ((0, 4),))
    return dict(queries=queries, key_states=key_states, value_states=value_states, doc_lengths=doc_lengths, move_plan=move_plan, expert_ids=expert_ids, gate_weights=gate_weights, expert_weight=expert_weight)


def token_starts(row_lengths, row_count):
    bounds = jnp.cumsum(row_lengths).astype(jnp.int32)
    positions = jnp.arange(row_count, dtype=jnp.int32)
    return jnp.max(jnp.where(bounds[None, :] <= positions[:, None], bounds[None, :], 0), axis=1)


def attend_row(inputs):
    query_rows, key_rows, value_rows, row_lengths = inputs
    starts = token_starts(row_lengths, ROW_TOKENS)
    positions = jnp.arange(ROW_TOKENS, dtype=jnp.int32)
    query_heads = query_rows.astype(jnp.float32).reshape(ROW_TOKENS, HEADS, HEAD_DIM)
    key_heads = key_rows.astype(jnp.float32).reshape(ROW_TOKENS, HEADS, HEAD_DIM)
    value_heads = value_rows.astype(jnp.float32).reshape(ROW_TOKENS, HEADS, HEAD_DIM)
    scores = jnp.einsum("qhd,khd->hqk", query_heads, key_heads) * (HEAD_DIM ** -0.5)
    allowed = (positions[None, :] <= positions[:, None]) & (positions[None, :] >= starts[:, None])
    scores = jnp.where(allowed[None], scores, -jnp.inf)
    weights = jax.nn.softmax(scores, axis=-1).astype(jnp.bfloat16)
    output = jnp.einsum("hqk,khd->qhd", weights.astype(jnp.float32), value_heads)
    return output.reshape(ROW_TOKENS, D_ATT).astype(jnp.bfloat16)


def reference(queries, key_states, value_states, doc_lengths, move_plan, expert_ids, gate_weights, expert_weight):
    attended = lax.map(attend_row, (queries.reshape(N_DP, ROW_TOKENS, D_ATT), key_states.reshape(N_DP, ROW_TOKENS, D_ATT), value_states.reshape(N_DP, ROW_TOKENS, D_ATT), doc_lengths))
    attended = attended.reshape(TOKENS, D_ATT)

    starts = jax.vmap(lambda lengths_row: token_starts(lengths_row, ROW_TOKENS))(doc_lengths)
    positions = jnp.arange(ROW_TOKENS, dtype=jnp.int32)
    pairs = (positions[None, :] - starts + 1).reshape(N_DP, BLOCKS, QBLOCK).sum(axis=2)
    row_ids = jnp.arange(N_DP, dtype=jnp.int32)
    runner = jnp.where(jnp.arange(BLOCKS, dtype=jnp.int32)[None, :] == move_plan[:, 1:2], move_plan[:, 0:1], row_ids[:, None])
    work = jax.ops.segment_sum(pairs.reshape(-1), runner.reshape(-1).astype(jnp.int32), N_DP)
    row_load = work.astype(jnp.float32) / (QBLOCK * QBLOCK)

    padded = jnp.concatenate([attended, jnp.zeros((1, D_ATT), jnp.bfloat16)], 0)

    def expert_step(carry, expert):
        chosen = expert_ids == expert
        picked = jnp.nonzero(jnp.any(chosen, axis=1), size=CAP * N_DP, fill_value=TOKENS)[0].astype(jnp.int32)
        weight_rows = jnp.sum(jnp.where(chosen, gate_weights, 0.0), axis=1)
        weight_rows = jnp.concatenate([weight_rows, jnp.zeros((1,), weight_rows.dtype)])
        pre_act = jnp.dot(padded[picked], expert_weight[expert], preferred_element_type=jnp.float32)
        rounded = lax.optimization_barrier(jax.nn.silu(pre_act).astype(jnp.bfloat16))
        activated = rounded.astype(jnp.float32)
        return carry.at[picked].add(weight_rows[picked][:, None] * activated), None

    summed, _ = lax.scan(expert_step, jnp.zeros((TOKENS + 1, EXPERT_FF), jnp.float32), jnp.arange(EXPERTS, dtype=jnp.int32))
    combined = summed[:TOKENS].astype(jnp.bfloat16)
    return (attended, combined, row_load)
```

```python
import functools

import jax
import jax.numpy as jnp
from jax import lax
from jax.experimental import pallas as pl
from jax.experimental.pallas import tpu as pltpu
from jax.sharding import PartitionSpec as P

HEAD_DIM = 128
QBLOCK = 128
MESH = pl.DeviceIdType.MESH
LOG2E = 1.4426950408889634


def span_pairs(low, high, start, stop):
    first = jnp.maximum(low, start)
    last = jnp.minimum(high, stop)
    count = jnp.maximum(last - first, 0)
    return (count * ((first - start + 1) + (last - start))) // 2


def row_pairs(lens, row, block, docs, row_count):
    low = block * QBLOCK
    total = jnp.int32(0)
    picked = jnp.int32(0)
    edge = jnp.int32(0)
    for doc in range(docs):
        stop = edge + lens[row, doc]
        total = total + span_pairs(0, row_count, edge, stop)
        picked = picked + span_pairs(low, low + QBLOCK, edge, stop)
        edge = stop
    return total, picked


def kernel(dp_size, group, q_hbm, k_hbm, v_hbm, lens, plan, ids, gates, w_hbm,
           att_hbm, comb, load,
           qv, kv, vv, wv, xg, acc, bias, gsc, part, rxd, txx, rxx,
           in_sem, w_sem, out_sem,
           sx_sem, rx_sem, sd_sem, rd_sem, sf_sem, rf_sem,
           ps_sem, pr_sem, qs_sem, qr_sem):
    rows, width = q_hbm.shape
    experts, depth, ff = w_hbm.shape
    chips = group // 2
    ck = qv.shape[1] // att_chunks(width)
    chunks = width // ck
    chip_width = 2 * width
    step_width = 2 * ck
    owned = ff // group
    row = lax.axis_index("dp")
    me = lax.axis_index("expert")
    chip = me // 2
    core = lax.rem(me, 2)
    other = chip * 2 + 1 - core

    def in_copies(c):
        cols = pl.ds(pl.multiple_of(c * ck, 128), ck)
        return [
            pltpu.make_async_copy(src.at[:, cols], dst.at[:, cols], in_sem.at[i, c])
            for i, (src, dst) in enumerate(((q_hbm, qv), (k_hbm, kv), (v_hbm, vv)))
        ]

    def place(s, c, k):
        return pl.multiple_of(s * chip_width + c * step_width + k * ck, 128)

    def w_copy(e, s, c, k):
        src = pl.multiple_of((s * 2 + k) * width + c * ck, 128)
        return pltpu.make_async_copy(
            w_hbm.at[e, pl.ds(src, ck), :], wv.at[e, pl.ds(place(s, c, k), ck), :],
            w_sem.at[e, s, c, k])

    def w_start(e, s, c):
        for k in range(2):
            w_copy(e, s, c, k).start()

    def w_wait(e, s, c):
        for k in range(2):
            w_copy(e, s, c, k).wait()

    for c in range(chunks):
        for copy in in_copies(c):
            copy.start()

    barrier = pltpu.get_barrier_semaphore()
    pl.semaphore_signal(barrier, inc=1, device_id={"expert": other}, device_id_type=MESH)
    for d in range(1, chips):
        peer = lax.rem(chip + d, chips) * 2 + core
        pl.semaphore_signal(barrier, inc=1, device_id={"expert": peer}, device_id_type=MESH)

    def start_own(i, _):
        w_start(i // chunks, chip, lax.rem(i, chunks))
        return 0

    lax.fori_loop(0, experts * chunks, start_own, 0)
    for d in range(1, chips):
        def start_far(i, _, d=d):
            w_start(lax.rem(i, experts), lax.rem(chip - d + chips, chips), i // experts)
            return 0

        lax.fori_loop(0, experts * chunks, start_far, 0)

    partner = lax.rem(row + dp_size // 2, dp_size)
    docs = lens.shape[1]
    own_total, own_moved = row_pairs(lens, row, plan[row, 1], docs, rows)
    _, their_moved = row_pairs(lens, partner, plan[partner, 1], docs, rows)
    work = own_total - jnp.where(plan[row, 0] != row, own_moved, 0)
    work = work + jnp.where(plan[partner, 0] != partner, their_moved, 0)
    load[0] = work.astype(jnp.float32) * (1.0 / (QBLOCK * QBLOCK))

    pos = lax.broadcasted_iota(jnp.int32, (rows, rows), 0)
    key_pos = lax.broadcasted_iota(jnp.int32, (rows, rows), 1)
    column = lax.broadcasted_iota(jnp.int32, (rows, 1), 0)
    starts = jnp.zeros((rows, 1), jnp.int32)
    edge = jnp.int32(0)
    for doc in range(docs):
        edge = edge + lens[row, doc]
        starts = jnp.where(column >= edge, jnp.maximum(starts, edge), starts)
    bias[...] = jnp.where((key_pos <= pos) & (key_pos >= starts), 0.0, -1e30)
    for e in range(experts):
        chosen = ids[...] == me * experts + e
        gsc[e] = jnp.sum(jnp.where(chosen, gates[...], 0.0), axis=1, keepdims=True)

    pl.semaphore_wait(barrier, chips)

    def cross_copy(c, d):
        cols = pl.ds(place(chip, c, core), ck)
        return pltpu.make_async_remote_copy(
            src_ref=xg.at[:, cols], dst_ref=xg.at[:, cols],
            send_sem=sx_sem.at[d - 1, c], recv_sem=rx_sem.at[d - 1, c],
            device_id={"expert": lax.rem(chip + d, chips) * 2 + core}, device_id_type=MESH)

    def side_copy(c):
        cols = pl.ds(place(chip, c, core), ck)
        return pltpu.make_async_remote_copy(
            src_ref=xg.at[:, cols], dst_ref=xg.at[:, cols],
            send_sem=sd_sem.at[c], recv_sem=rd_sem.at[c],
            device_id={"expert": other}, device_id_type=MESH)

    def pass_copy(c, d):
        cols = pl.ds(place(lax.rem(chip - d + chips, chips), c, core), ck)
        return pltpu.make_async_remote_copy(
            src_ref=xg.at[:, cols], dst_ref=xg.at[:, cols],
            send_sem=sf_sem.at[d - 1, c], recv_sem=rf_sem.at[d - 1, c],
            device_id={"expert": other}, device_id_type=MESH)

    def out_copy(c):
        return pltpu.make_async_copy(
            xg.at[:, pl.ds(place(chip, c, core), ck)],
            att_hbm.at[:, pl.ds(pl.multiple_of(c * ck, 128), ck)], out_sem.at[c])

    scale = HEAD_DIM ** -0.5 * LOG2E
    qb = rows // 2

    def attend(c, _):
        for copy in in_copies(c):
            copy.wait()
        for h in range(ck // HEAD_DIM):
            cols = pl.ds(pl.multiple_of(c * ck + h * HEAD_DIM, 128), HEAD_DIM)
            dst = pl.ds(pl.multiple_of(place(chip, c, core) + h * HEAD_DIM, 128), HEAD_DIM)
            for b in range(2):
                low, high = b * qb, (b + 1) * qb
                s = lax.dot_general(
                    qv[low:high, cols], kv[:high, cols], (((1,), (1,)), ((), ())),
                    preferred_element_type=jnp.float32)
                s = s + bias[low:high, :high]
                top = jnp.max(s, axis=1, keepdims=True)
                p = jnp.exp2((s - top) * scale)
                norm = jnp.sum(p, axis=1, keepdims=True)
                o = jnp.dot(p.astype(jnp.bfloat16), vv[:high, cols],
                            preferred_element_type=jnp.float32)
                xg[low:high, dst] = (o / norm).astype(jnp.bfloat16)
        for d in range(1, chips):
            cross_copy(c, d).start()
        side_copy(c).start()
        out_copy(c).start()
        return 0

    lax.fori_loop(0, chunks, attend, 0)

    forwards = [(c, d) for c in range(chunks) for d in range(1, chips)]
    sent = [0]

    def forward(count):
        while sent[0] < min(count, len(forwards)):
            c, d = forwards[sent[0]]
            cross_copy(c, d).wait_recv()
            pass_copy(c, d).start()
            sent[0] += 1

    for c in range(chunks):
        side_copy(c).wait_recv()
    own = pl.ds(pl.multiple_of(chip * chip_width, 128), chip_width)
    tile = ff // 2
    for e in range(experts):
        def wait_own(c, _, e=e):
            w_wait(e, chip, c)
            return 0

        lax.fori_loop(0, chunks, wait_own, 0)

        def near(t, _, e=e):
            cols = pl.ds(pl.multiple_of(t * tile, 128), tile)
            acc[e, :, cols] = jnp.dot(xg[:, own], wv[e, own, cols],
                                      preferred_element_type=jnp.float32)
            return 0

        lax.fori_loop(0, 2, near, 0)
        if e == 0 or e == experts - 2:
            forward(sent[0] + 1)

    for i, (c, d) in enumerate(forwards):
        last = i == len(forwards) - 1
        forward(i + 2 if i + 2 < len(forwards) else i + 1)
        src = lax.rem(chip - d + chips, chips)
        pass_copy(c, d).wait_recv()
        span = pl.ds(place(src, c, 0), step_width)

        def wait_far(e, _, src=src, c=c):
            w_wait(e, src, c)
            return 0

        lax.fori_loop(0, experts, wait_far, 0)
        if not last:
            def far(e, _, span=span):
                acc[e] += jnp.dot(xg[:, span], wv[e, span, :],
                                  preferred_element_type=jnp.float32)
                return 0

            lax.fori_loop(0, experts, far, 0)
            if i + 2 == len(forwards):
                forward(len(forwards))

    def pair_copy(j):
        return pltpu.make_async_remote_copy(
            src_ref=part.at[j * 2 + 1 - core], dst_ref=rxd.at[j],
            send_sem=ps_sem.at[j], recv_sem=pr_sem.at[j],
            device_id={"expert": other}, device_id_type=MESH)

    def sum_copy(d):
        return pltpu.make_async_remote_copy(
            src_ref=txx.at[d - 1], dst_ref=rxx.at[d - 1],
            send_sem=qs_sem.at[d - 1], recv_sem=qr_sem.at[d - 1],
            device_id={"expert": lax.rem(chip + d, chips) * 2 + core}, device_id_type=MESH)

    c, d = forwards[-1]
    span = pl.ds(place(lax.rem(chip - d + chips, chips), c, 0), step_width)
    band = 2 * owned
    rt = 64
    for d in list(range(1, chips)) + [0]:
        j = lax.rem(chip + d, chips)
        cols = pl.ds(pl.multiple_of(j * band, 128), band)
        for e in range(experts):
            acc[e, :, cols] += jnp.dot(xg[:, span], wv[e, span, cols],
                                       preferred_element_type=jnp.float32)

        def finish(r, _, cols=cols, j=j):
            at = pl.ds(pl.multiple_of(r * rt, rt), rt)
            total = jnp.zeros((rt, band), jnp.float32)
            for e in range(experts):
                half = acc[e, at, cols] * 0.5
                total = total + (half * jnp.tanh(half) + half) * gsc[e, at, :]
            total = total.astype(jnp.bfloat16)
            part[j * 2, at, :] = total[:, :owned]
            part[j * 2 + 1, at, :] = total[:, owned:]
            return 0

        lax.fori_loop(0, rows // rt, finish, 0)
        pair_copy(j).start()

    for d in range(1, chips):
        j = lax.rem(chip + d, chips)
        pair_copy(j).wait_recv()
        txx[d - 1] = (part[j * 2 + core].astype(jnp.float32)
                      + rxd[j].astype(jnp.float32)).astype(jnp.bfloat16)
        sum_copy(d).start()
    pair_copy(chip).wait_recv()
    total = part[chip * 2 + core].astype(jnp.float32) + rxd[chip].astype(jnp.float32)
    for d in range(1, chips):
        sum_copy(d).wait_recv()
        total = total + rxx[d - 1].astype(jnp.float32)
    comb[...] = total.astype(jnp.bfloat16)

    for c in range(chunks):
        out_copy(c).wait()
        side_copy(c).wait_send()
        for d in range(1, chips):
            cross_copy(c, d).wait_send()
            pass_copy(c, d).wait_send()
    for j in range(chips):
        pair_copy(j).wait_send()
    for d in range(1, chips):
        sum_copy(d).wait_send()


def att_chunks(width):
    return width // (2 * HEAD_DIM)


def shards(dp_size, group, queries, key_states, value_states, doc_lengths, move_plan,
           expert_ids, gate_weights, expert_weight):
    rows, width = queries.shape
    experts, depth, ff = expert_weight.shape
    chips = group // 2
    chunks = att_chunks(width)
    owned = ff // group
    bf16, f32 = jnp.bfloat16, jnp.float32
    hbm = pl.BlockSpec(memory_space=pl.ANY)
    smem = pl.BlockSpec(memory_space=pltpu.SMEM)
    vmem = pl.BlockSpec(memory_space=pltpu.VMEM)
    dma = pltpu.SemaphoreType.DMA
    return pl.pallas_call(
        functools.partial(kernel, dp_size, group),
        out_shape=(
            jax.ShapeDtypeStruct((rows, width), bf16),
            jax.ShapeDtypeStruct((rows, owned), bf16),
            jax.ShapeDtypeStruct((1,), f32),
        ),
        in_specs=[hbm, hbm, hbm, smem, smem, vmem, vmem, hbm],
        out_specs=(hbm, vmem, smem),
        scratch_shapes=[
            pltpu.VMEM((rows, width), bf16),
            pltpu.VMEM((rows, width), bf16),
            pltpu.VMEM((rows, width), bf16),
            pltpu.VMEM((experts, depth, ff), bf16),
            pltpu.VMEM((rows, depth), bf16),
            pltpu.VMEM((experts, rows, ff), f32),
            pltpu.VMEM((rows, rows), f32),
            pltpu.VMEM((experts, rows, 1), f32),
            pltpu.VMEM((group, rows, owned), bf16),
            pltpu.VMEM((chips, rows, owned), bf16),
            pltpu.VMEM((chips - 1, rows, owned), bf16),
            pltpu.VMEM((chips - 1, rows, owned), bf16),
            dma((3, chunks)),
            dma((experts, chips, chunks, 2)),
            dma((chunks,)),
            dma((chips - 1, chunks)),
            dma((chips - 1, chunks)),
            dma((chunks,)),
            dma((chunks,)),
            dma((chips - 1, chunks)),
            dma((chips - 1, chunks)),
            dma((chips,)),
            dma((chips,)),
            dma((chips - 1,)),
            dma((chips - 1,)),
        ],
        compiler_params=pltpu.CompilerParams(
            collective_id=0, has_side_effects=True, vmem_limit_bytes=66_000_000),
    )(queries, key_states, value_states, doc_lengths, move_plan, expert_ids, gate_weights,
      expert_weight)


def solution(mesh):
    in_specs = (
        P("dp", "expert"),
        P("dp", "expert"),
        P("dp", "expert"),
        P(),
        P(),
        P("dp", None),
        P("dp", None),
        P("expert", None, None),
    )
    out_specs = (P("dp", "expert"), P("dp", "expert"), P("dp"))
    body = functools.partial(shards, mesh.shape["dp"], mesh.shape["expert"])
    return jax.shard_map(body, mesh=mesh, in_specs=in_specs, out_specs=out_specs, check_vma=False)
```

```python
import functools

import jax
import jax.numpy as jnp
from jax import lax
from jax.experimental import pallas as pl
from jax.experimental.pallas import tpu as pltpu
from jax.sharding import PartitionSpec as P

HEAD_DIM = 128
QBLOCK = 128
MESH = pl.DeviceIdType.MESH
LOG2E = 1.4426950408889634


def span_pairs(low, high, start, stop):
    first = jnp.maximum(low, start)
    last = jnp.minimum(high, stop)
    count = jnp.maximum(last - first, 0)
    return (count * ((first - start + 1) + (last - start))) // 2


def row_pairs(lens, row, block, docs, row_count):
    low = block * QBLOCK
    total = jnp.int32(0)
    picked = jnp.int32(0)
    edge = jnp.int32(0)
    for doc in range(docs):
        stop = edge + lens[row, doc]
        total = total + span_pairs(0, row_count, edge, stop)
        picked = picked + span_pairs(low, low + QBLOCK, edge, stop)
        edge = stop
    return total, picked


def kernel(dp_size, group, q_hbm, k_hbm, v_hbm, lens, plan, ids, gates, w_hbm,
           att_hbm, comb, load,
           qv, kv, vv, wv, xg, acc, bias, gsc, part, rxd, txx, rxx,
           in_sem, w_sem, out_sem,
           sx_sem, rx_sem, sd_sem, rd_sem, sf_sem, rf_sem,
           ps_sem, pr_sem, qs_sem, qr_sem):
    rows, width = q_hbm.shape
    experts, depth, ff = w_hbm.shape
    chips = group // 2
    ck = qv.shape[1] // att_chunks(width)
    chunks = width // ck
    chip_width = 2 * width
    step_width = 2 * ck
    owned = ff // group
    row = lax.axis_index("dp")
    me = lax.axis_index("expert")
    chip = me // 2
    core = lax.rem(me, 2)
    other = chip * 2 + 1 - core

    def in_copies(c):
        cols = pl.ds(pl.multiple_of(c * ck, 128), ck)
        return [
            pltpu.make_async_copy(src.at[:, cols], dst.at[:, cols], in_sem.at[i, c])
            for i, (src, dst) in enumerate(((q_hbm, qv), (k_hbm, kv), (v_hbm, vv)))
        ]

    def place(s, c, k):
        return pl.multiple_of(s * chip_width + c * step_width + k * ck, 128)

    def w_copy(e, s, c, k):
        src = pl.multiple_of((s * 2 + k) * width + c * ck, 128)
        return pltpu.make_async_copy(
            w_hbm.at[e, pl.ds(src, ck), :], wv.at[e, pl.ds(place(s, c, k), ck), :],
            w_sem.at[e, s, c, k])

    def w_start(e, s, c):
        for k in range(2):
            w_copy(e, s, c, k).start()

    def w_wait(e, s, c):
        for k in range(2):
            w_copy(e, s, c, k).wait()

    for c in range(chunks):
        for copy in in_copies(c):
            copy.start()

    barrier = pltpu.get_barrier_semaphore()
    pl.semaphore_signal(barrier, inc=1, device_id={"expert": other}, device_id_type=MESH)
    for d in range(1, chips):
        peer = lax.rem(chip + d, chips) * 2 + core
        pl.semaphore_signal(barrier, inc=1, device_id={"expert": peer}, device_id_type=MESH)

    def start_own(i, _):
        w_start(i // chunks, chip, lax.rem(i, chunks))
        return 0

    lax.fori_loop(0, experts * chunks, start_own, 0)
    docs = lens.shape[1]
    pos = lax.broadcasted_iota(jnp.int32, (rows, rows), 0)
    key_pos = lax.broadcasted_iota(jnp.int32, (rows, rows), 1)
    column = lax.broadcasted_iota(jnp.int32, (rows, 1), 0)
    starts = jnp.zeros((rows, 1), jnp.int32)
    edge = jnp.int32(0)
    for doc in range(docs):
        edge = edge + lens[row, doc]
        starts = jnp.where(column >= edge, jnp.maximum(starts, edge), starts)
    bias[...] = jnp.where((key_pos <= pos) & (key_pos >= starts), 0.0, -1e30)

    pl.semaphore_wait(barrier, chips)

    def cross_copy(c, d):
        cols = pl.ds(place(chip, c, core), ck)
        return pltpu.make_async_remote_copy(
            src_ref=xg.at[:, cols], dst_ref=xg.at[:, cols],
            send_sem=sx_sem.at[d - 1, c], recv_sem=rx_sem.at[d - 1, c],
            device_id={"expert": lax.rem(chip + d, chips) * 2 + core}, device_id_type=MESH)

    def side_copy(c):
        cols = pl.ds(place(chip, c, core), ck)
        return pltpu.make_async_remote_copy(
            src_ref=xg.at[:, cols], dst_ref=xg.at[:, cols],
            send_sem=sd_sem.at[c], recv_sem=rd_sem.at[c],
            device_id={"expert": other}, device_id_type=MESH)

    def pass_copy(c, d):
        cols = pl.ds(place(lax.rem(chip - d + chips, chips), c, core), ck)
        return pltpu.make_async_remote_copy(
            src_ref=xg.at[:, cols], dst_ref=xg.at[:, cols],
            send_sem=sf_sem.at[d - 1, c], recv_sem=rf_sem.at[d - 1, c],
            device_id={"expert": other}, device_id_type=MESH)

    def out_copy(c):
        return pltpu.make_async_copy(
            xg.at[:, pl.ds(place(chip, c, core), ck)],
            att_hbm.at[:, pl.ds(pl.multiple_of(c * ck, 128), ck)], out_sem.at[c])

    scale = HEAD_DIM ** -0.5 * LOG2E
    qb = rows // 2

    def attend(c, _):
        for copy in in_copies(c):
            copy.wait()
        for h in range(ck // HEAD_DIM):
            cols = pl.ds(pl.multiple_of(c * ck + h * HEAD_DIM, 128), HEAD_DIM)
            dst = pl.ds(pl.multiple_of(place(chip, c, core) + h * HEAD_DIM, 128), HEAD_DIM)
            for b in range(2):
                low, high = b * qb, (b + 1) * qb
                s = lax.dot_general(
                    qv[low:high, cols], kv[:high, cols], (((1,), (1,)), ((), ())),
                    preferred_element_type=jnp.float32)
                s = s + bias[low:high, :high]
                top = jnp.max(s, axis=1, keepdims=True)
                p = jnp.exp2((s - top) * scale)
                norm = jnp.sum(p, axis=1, keepdims=True)
                o = jnp.dot(p.astype(jnp.bfloat16), vv[:high, cols],
                            preferred_element_type=jnp.float32)
                xg[low:high, dst] = (o / norm).astype(jnp.bfloat16)
        for d in range(1, chips):
            cross_copy(c, d).start()
        side_copy(c).start()
        out_copy(c).start()
        return 0

    lax.fori_loop(0, chunks, attend, 0)

    for d in range(1, chips):
        def start_far(i, _, d=d):
            w_start(lax.rem(i, experts), lax.rem(chip - d + chips, chips), i // experts)
            return 0

        lax.fori_loop(0, experts * chunks, start_far, 0)

    partner = lax.rem(row + dp_size // 2, dp_size)
    own_total, own_moved = row_pairs(lens, row, plan[1, row], docs, rows)
    _, their_moved = row_pairs(lens, partner, plan[1, partner], docs, rows)
    work = own_total - jnp.where(plan[0, row] != row, own_moved, 0)
    work = work + jnp.where(plan[0, partner] != partner, their_moved, 0)
    load[0] = work.astype(jnp.float32) * (1.0 / (QBLOCK * QBLOCK))

    for e in range(experts):
        chosen = ids[...] == me * experts + e
        line = jnp.sum(jnp.where(chosen, gates[...], 0.0), axis=0, keepdims=True)
        for r in range(0, rows, 128):
            gsc[e, r:r + 128, :] = jnp.broadcast_to(line[:, r:r + 128], (128, 128)).T

    forwards = [(c, d) for c in range(chunks) for d in range(1, chips)]
    sent = [0]

    def forward(count):
        while sent[0] < min(count, len(forwards)):
            c, d = forwards[sent[0]]
            cross_copy(c, d).wait_recv()
            pass_copy(c, d).start()
            sent[0] += 1

    for c in range(chunks):
        side_copy(c).wait_recv()
    own = pl.ds(pl.multiple_of(chip * chip_width, 128), chip_width)
    tile = ff // 2
    for e in range(experts):
        def wait_own(c, _, e=e):
            w_wait(e, chip, c)
            return 0

        lax.fori_loop(0, chunks, wait_own, 0)

        def near(t, _, e=e):
            cols = pl.ds(pl.multiple_of(t * tile, 128), tile)
            acc[e, :, cols] = jnp.dot(xg[:, own], wv[e, own, cols],
                                      preferred_element_type=jnp.float32)
            return 0

        lax.fori_loop(0, 2, near, 0)
        if e == 0 or e == experts - 2:
            forward(sent[0] + 1)

    for i, (c, d) in enumerate(forwards):
        last = i == len(forwards) - 1
        forward(i + 2 if i + 2 < len(forwards) else i + 1)
        src = lax.rem(chip - d + chips, chips)
        pass_copy(c, d).wait_recv()
        span = pl.ds(place(src, c, 0), step_width)

        def wait_far(e, _, src=src, c=c):
            w_wait(e, src, c)
            return 0

        lax.fori_loop(0, experts, wait_far, 0)
        if not last:
            def far(e, _, span=span):
                acc[e] += jnp.dot(xg[:, span], wv[e, span, :],
                                  preferred_element_type=jnp.float32)
                return 0

            lax.fori_loop(0, experts, far, 0)
            if i + 2 == len(forwards):
                forward(len(forwards))

    def pair_copy(j):
        return pltpu.make_async_remote_copy(
            src_ref=part.at[j * 2 + 1 - core], dst_ref=rxd.at[j],
            send_sem=ps_sem.at[j], recv_sem=pr_sem.at[j],
            device_id={"expert": other}, device_id_type=MESH)

    def sum_copy(d):
        return pltpu.make_async_remote_copy(
            src_ref=txx.at[d - 1], dst_ref=rxx.at[d - 1],
            send_sem=qs_sem.at[d - 1], recv_sem=qr_sem.at[d - 1],
            device_id={"expert": lax.rem(chip + d, chips) * 2 + core}, device_id_type=MESH)

    c, d = forwards[-1]
    span = pl.ds(place(lax.rem(chip - d + chips, chips), c, 0), step_width)
    band = 2 * owned
    rt = 64
    for d in list(range(1, chips)) + [0]:
        j = lax.rem(chip + d, chips)
        cols = pl.ds(pl.multiple_of(j * band, 128), band)
        for e in range(experts):
            acc[e, :, cols] += jnp.dot(xg[:, span], wv[e, span, cols],
                                       preferred_element_type=jnp.float32)

        def finish(r, _, cols=cols, j=j):
            at = pl.ds(pl.multiple_of(r * rt, rt), rt)
            total = jnp.zeros((rt, band), jnp.float32)
            for e in range(experts):
                half = acc[e, at, cols] * 0.5
                total = total + (half * jnp.tanh(half) + half) * jnp.concatenate(
                    [gsc[e, at, :]] * (band // 128), axis=1)
            total = total.astype(jnp.bfloat16)
            part[j * 2, at, :] = total[:, :owned]
            part[j * 2 + 1, at, :] = total[:, owned:]
            return 0

        lax.fori_loop(0, rows // rt, finish, 0)
        pair_copy(j).start()

    for d in range(1, chips):
        j = lax.rem(chip + d, chips)
        pair_copy(j).wait_recv()
        txx[d - 1] = (part[j * 2 + core].astype(jnp.float32)
                      + rxd[j].astype(jnp.float32)).astype(jnp.bfloat16)
        sum_copy(d).start()
    pair_copy(chip).wait_recv()
    total = part[chip * 2 + core].astype(jnp.float32) + rxd[chip].astype(jnp.float32)
    for d in range(1, chips):
        sum_copy(d).wait_recv()
        total = total + rxx[d - 1].astype(jnp.float32)
    comb[...] = total.astype(jnp.bfloat16)

    for c in range(chunks):
        out_copy(c).wait()
        side_copy(c).wait_send()
        for d in range(1, chips):
            cross_copy(c, d).wait_send()
            pass_copy(c, d).wait_send()
    for j in range(chips):
        pair_copy(j).wait_send()
    for d in range(1, chips):
        sum_copy(d).wait_send()


def att_chunks(width):
    return width // (2 * HEAD_DIM)


def shards(dp_size, group, queries, key_states, value_states, doc_lengths, move_plan,
           expert_ids, gate_weights, expert_weight):
    rows, width = queries.shape
    experts, depth, ff = expert_weight.shape
    chips = group // 2
    chunks = att_chunks(width)
    owned = ff // group
    bf16, f32 = jnp.bfloat16, jnp.float32
    hbm = pl.BlockSpec(memory_space=pl.ANY)
    smem = pl.BlockSpec(memory_space=pltpu.SMEM)
    vmem = pl.BlockSpec(memory_space=pltpu.VMEM)
    dma = pltpu.SemaphoreType.DMA
    return pl.pallas_call(
        functools.partial(kernel, dp_size, group),
        out_shape=(
            jax.ShapeDtypeStruct((rows, width), bf16),
            jax.ShapeDtypeStruct((rows, owned), bf16),
            jax.ShapeDtypeStruct((1,), f32),
        ),
        in_specs=[hbm, hbm, hbm, smem, smem, vmem, vmem, hbm],
        out_specs=(hbm, vmem, smem),
        scratch_shapes=[
            pltpu.VMEM((rows, width), bf16),
            pltpu.VMEM((rows, width), bf16),
            pltpu.VMEM((rows, width), bf16),
            pltpu.VMEM((experts, depth, ff), bf16),
            pltpu.VMEM((rows, depth), bf16),
            pltpu.VMEM((experts, rows, ff), f32),
            pltpu.VMEM((rows, rows), f32),
            pltpu.VMEM((experts, rows, 128), f32),
            pltpu.VMEM((group, rows, owned), bf16),
            pltpu.VMEM((chips, rows, owned), bf16),
            pltpu.VMEM((chips - 1, rows, owned), bf16),
            pltpu.VMEM((chips - 1, rows, owned), bf16),
            dma((3, chunks)),
            dma((experts, chips, chunks, 2)),
            dma((chunks,)),
            dma((chips - 1, chunks)),
            dma((chips - 1, chunks)),
            dma((chunks,)),
            dma((chunks,)),
            dma((chips - 1, chunks)),
            dma((chips - 1, chunks)),
            dma((chips,)),
            dma((chips,)),
            dma((chips - 1,)),
            dma((chips - 1,)),
        ],
        compiler_params=pltpu.CompilerParams(
            collective_id=0, has_side_effects=True, vmem_limit_bytes=66_000_000),
    )(queries, key_states, value_states, doc_lengths, move_plan.T, expert_ids.T,
      gate_weights.T, expert_weight)


def solution(mesh):
    in_specs = (
        P("dp", "expert"),
        P("dp", "expert"),
        P("dp", "expert"),
        P(),
        P(),
        P("dp", None),
        P("dp", None),
        P("expert", None, None),
    )
    out_specs = (P("dp", "expert"), P("dp", "expert"), P("dp"))
    body = functools.partial(shards, mesh.shape["dp"], mesh.shape["expert"])
    return jax.shard_map(body, mesh=mesh, in_specs=in_specs, out_specs=out_specs, check_vma=False)
```

```python
import functools

import jax
import jax.numpy as jnp
from jax import lax
from jax.experimental import pallas as pl
from jax.experimental.pallas import tpu as pltpu
from jax.sharding import PartitionSpec as P

HEAD_DIM = 128
QBLOCK = 128
MESH = pl.DeviceIdType.MESH
LOG2E = 1.4426950408889634


def span_pairs(low, high, start, stop):
    first = jnp.maximum(low, start)
    last = jnp.minimum(high, stop)
    count = jnp.maximum(last - first, 0)
    return (count * ((first - start + 1) + (last - start))) // 2


def row_pairs(lens, row, block, docs, row_count):
    low = block * QBLOCK
    total = jnp.int32(0)
    picked = jnp.int32(0)
    edge = jnp.int32(0)
    for doc in range(docs):
        stop = edge + lens[row, doc]
        total = total + span_pairs(0, row_count, edge, stop)
        picked = picked + span_pairs(low, low + QBLOCK, edge, stop)
        edge = stop
    return total, picked


def kernel(dp_size, group, q_hbm, k_hbm, v_hbm, lens, plan, ids, gates, w_hbm,
           att_hbm, comb, load,
           qv, kv, vv, wv, xg, acc, bias, gsc, part, rxd, txx, rxx,
           in_sem, w_sem, out_sem,
           sx_sem, rx_sem, sd_sem, rd_sem, sf_sem, rf_sem,
           ps_sem, pr_sem, qs_sem, qr_sem):
    rows, width = q_hbm.shape
    experts, depth, ff = w_hbm.shape
    chips = group // 2
    ck = qv.shape[1] // att_chunks(width)
    chunks = width // ck
    chip_width = 2 * width
    step_width = 2 * ck
    owned = ff // group
    row = lax.axis_index("dp")
    me = lax.axis_index("expert")
    chip = me // 2
    core = lax.rem(me, 2)
    other = chip * 2 + 1 - core

    def in_copies(c):
        cols = pl.ds(pl.multiple_of(c * ck, 128), ck)
        return [
            pltpu.make_async_copy(src.at[:, cols], dst.at[:, cols], in_sem.at[i, c])
            for i, (src, dst) in enumerate(((q_hbm, qv), (k_hbm, kv), (v_hbm, vv)))
        ]

    def place(s, c, k):
        return pl.multiple_of(s * chip_width + c * step_width + k * ck, 128)

    def w_copy(e, s, c, k):
        src = pl.multiple_of((s * 2 + k) * width + c * ck, 128)
        return pltpu.make_async_copy(
            w_hbm.at[e, pl.ds(src, ck), :], wv.at[e, pl.ds(place(s, c, k), ck), :],
            w_sem.at[e, s, c, k])

    def w_start(e, s, c):
        for k in range(2):
            w_copy(e, s, c, k).start()

    def w_wait(e, s, c):
        for k in range(2):
            w_copy(e, s, c, k).wait()

    for c in range(chunks):
        for copy in in_copies(c):
            copy.start()

    barrier = pltpu.get_barrier_semaphore()
    pl.semaphore_signal(barrier, inc=1, device_id={"expert": other}, device_id_type=MESH)
    for d in range(1, chips):
        peer = lax.rem(chip + d, chips) * 2 + core
        pl.semaphore_signal(barrier, inc=1, device_id={"expert": peer}, device_id_type=MESH)

    def start_own(i, _):
        w_start(i // chunks, chip, lax.rem(i, chunks))
        return 0

    lax.fori_loop(0, experts * chunks, start_own, 0)
    docs = lens.shape[1]
    pos = lax.broadcasted_iota(jnp.int32, (rows, rows), 0)
    key_pos = lax.broadcasted_iota(jnp.int32, (rows, rows), 1)
    column = lax.broadcasted_iota(jnp.int32, (rows, 1), 0)
    starts = jnp.zeros((rows, 1), jnp.int32)
    edge = jnp.int32(0)
    for doc in range(docs):
        edge = edge + lens[row, doc]
        starts = jnp.where(column >= edge, jnp.maximum(starts, edge), starts)
    bias[...] = jnp.where((key_pos <= pos) & (key_pos >= starts), 0.0, -1e30)

    pl.semaphore_wait(barrier, chips)

    half = rows // 2

    def band_of(b):
        return pl.ds(b * half, half)

    def cross_copy(b, c, d):
        at = xg.at[band_of(b), pl.ds(place(chip, c, core), ck)]
        return pltpu.make_async_remote_copy(
            src_ref=at, dst_ref=at,
            send_sem=sx_sem.at[d - 1, b, c], recv_sem=rx_sem.at[d - 1, b, c],
            device_id={"expert": lax.rem(chip + d, chips) * 2 + core}, device_id_type=MESH)

    def side_copy(b, c):
        at = xg.at[band_of(b), pl.ds(place(chip, c, core), ck)]
        return pltpu.make_async_remote_copy(
            src_ref=at, dst_ref=at,
            send_sem=sd_sem.at[b, c], recv_sem=rd_sem.at[b, c],
            device_id={"expert": other}, device_id_type=MESH)

    def pass_copy(b, c, d):
        at = xg.at[band_of(b), pl.ds(place(lax.rem(chip - d + chips, chips), c, core), ck)]
        return pltpu.make_async_remote_copy(
            src_ref=at, dst_ref=at,
            send_sem=sf_sem.at[d - 1, b, c], recv_sem=rf_sem.at[d - 1, b, c],
            device_id={"expert": other}, device_id_type=MESH)

    def out_copy(c):
        return pltpu.make_async_copy(
            xg.at[:, pl.ds(place(chip, c, core), ck)],
            att_hbm.at[:, pl.ds(pl.multiple_of(c * ck, 128), ck)], out_sem.at[c])

    scale = HEAD_DIM ** -0.5 * LOG2E

    for b in range(2):
        low, high = b * half, (b + 1) * half

        def attend(c, _, b=b, low=low, high=high):
            if b == 0:
                for copy in in_copies(c):
                    copy.wait()
            for h in range(ck // HEAD_DIM):
                cols = pl.ds(pl.multiple_of(c * ck + h * HEAD_DIM, 128), HEAD_DIM)
                dst = pl.ds(pl.multiple_of(place(chip, c, core) + h * HEAD_DIM, 128), HEAD_DIM)
                s = lax.dot_general(
                    qv[low:high, cols], kv[:high, cols], (((1,), (1,)), ((), ())),
                    preferred_element_type=jnp.float32)
                s = s + bias[low:high, :high]
                top = jnp.max(s, axis=1, keepdims=True)
                p = jnp.exp2((s - top) * scale)
                norm = jnp.sum(p, axis=1, keepdims=True)
                o = jnp.dot(p.astype(jnp.bfloat16), vv[:high, cols],
                            preferred_element_type=jnp.float32)
                xg[low:high, dst] = (o / norm).astype(jnp.bfloat16)
            for d in range(1, chips):
                cross_copy(b, c, d).start()
            side_copy(b, c).start()
            if b == 1:
                out_copy(c).start()
            return 0

        lax.fori_loop(0, chunks, attend, 0)

    for d in range(1, chips):
        def start_far(i, _, d=d):
            w_start(lax.rem(i, experts), lax.rem(chip - d + chips, chips), i // experts)
            return 0

        lax.fori_loop(0, experts * chunks, start_far, 0)

    partner = lax.rem(row + dp_size // 2, dp_size)
    own_total, own_moved = row_pairs(lens, row, plan[1, row], docs, rows)
    _, their_moved = row_pairs(lens, partner, plan[1, partner], docs, rows)
    work = own_total - jnp.where(plan[0, row] != row, own_moved, 0)
    work = work + jnp.where(plan[0, partner] != partner, their_moved, 0)
    load[0] = work.astype(jnp.float32) * (1.0 / (QBLOCK * QBLOCK))

    for e in range(experts):
        chosen = ids[...] == me * experts + e
        line = jnp.sum(jnp.where(chosen, gates[...], 0.0), axis=0, keepdims=True)
        for r in range(0, rows, 128):
            gsc[e, r:r + 128, :] = jnp.broadcast_to(line[:, r:r + 128], (128, 128)).T

    forwards = [(b, c, d) for b in range(2) for c in range(chunks) for d in range(1, chips)]
    per_half = len(forwards) // 2
    sent = [0]

    def forward(count):
        while sent[0] < min(count, len(forwards)):
            b, c, d = forwards[sent[0]]
            cross_copy(b, c, d).wait_recv()
            pass_copy(b, c, d).start()
            sent[0] += 1

    forward(1)
    for b in range(2):
        for c in range(chunks):
            side_copy(b, c).wait_recv()
    own = pl.ds(pl.multiple_of(chip * chip_width, 128), chip_width)
    tile = ff // 2
    for e in range(experts):
        def wait_own(c, _, e=e):
            w_wait(e, chip, c)
            return 0

        lax.fori_loop(0, chunks, wait_own, 0)

        def near(t, _, e=e):
            cols = pl.ds(pl.multiple_of(t * tile, 128), tile)
            acc[e, :, cols] = jnp.dot(xg[:, own], wv[e, own, cols],
                                      preferred_element_type=jnp.float32)
            return 0

        lax.fori_loop(0, 2, near, 0)
        forward(min(sent[0] + 1, per_half))

    def pair_copy(b, j):
        return pltpu.make_async_remote_copy(
            src_ref=part.at[j * 2 + 1 - core, band_of(b)], dst_ref=rxd.at[j, band_of(b)],
            send_sem=ps_sem.at[b, j], recv_sem=pr_sem.at[b, j],
            device_id={"expert": other}, device_id_type=MESH)

    def sum_copy(b, d):
        return pltpu.make_async_remote_copy(
            src_ref=txx.at[d - 1, band_of(b)], dst_ref=rxx.at[d - 1, band_of(b)],
            send_sem=qs_sem.at[b, d - 1], recv_sem=qr_sem.at[b, d - 1],
            device_id={"expert": lax.rem(chip + d, chips) * 2 + core}, device_id_type=MESH)

    def exchange(b):
        at = band_of(b)
        for d in range(1, chips):
            j = lax.rem(chip + d, chips)
            pair_copy(b, j).wait_recv()
            txx[d - 1, at, :] = (part[j * 2 + core, at, :].astype(jnp.float32)
                                 + rxd[j, at, :].astype(jnp.float32)).astype(jnp.bfloat16)
            sum_copy(b, d).start()

    def arrive(b, c0, c1, d):
        for c in range(c0, c1):
            forward(forwards.index((b, c, d)) + 1)
        for c in range(c0, c1):
            pass_copy(b, c, d).wait_recv()
            if b == 0:
                def wait_far(e, _, c=c, d=d):
                    w_wait(e, lax.rem(chip - d + chips, chips), c)
                    return 0

                lax.fori_loop(0, experts, wait_far, 0)
        return pl.ds(place(lax.rem(chip - d + chips, chips), c0, 0), (c1 - c0) * step_width)

    columns = 2 * owned
    rt = 64

    def add_far(b, e, span, cols):
        at = band_of(b)
        acc[e, at, cols] += jnp.dot(xg[at, span], wv[e, span, cols],
                                    preferred_element_type=jnp.float32)

    def close(b, span):
        for d in list(range(1, chips)) + [0]:
            j = lax.rem(chip + d, chips)
            cols = pl.ds(pl.multiple_of(j * columns, 128), columns)
            for e in range(experts):
                add_far(b, e, span, cols)

            def finish(r, _, cols=cols, j=j):
                at = pl.ds(pl.multiple_of(b * half + r * rt, rt), rt)
                total = jnp.zeros((rt, columns), jnp.float32)
                for e in range(experts):
                    h = acc[e, at, cols] * 0.5
                    total = total + (h * jnp.tanh(h) + h) * jnp.concatenate(
                        [gsc[e, at, :]] * (columns // 128), axis=1)
                total = total.astype(jnp.bfloat16)
                part[j * 2, at, :] = total[:, :owned]
                part[j * 2 + 1, at, :] = total[:, owned:]
                return 0

            lax.fori_loop(0, half // rt, finish, 0)
            pair_copy(b, j).start()

    whole = pl.ds(0, ff)
    for d in range(1, chips):
        span = arrive(0, 0, chunks, d)
        if d < chips - 1:
            for e in range(experts):
                add_far(0, e, span, whole)
    forward(per_half + 1)
    close(0, span)
    forward(per_half + 2)
    exchanged = False
    if chunks > 1:
        for d in range(1, chips):
            span = arrive(1, 0, chunks - 1, d)
            for e in range(experts):
                add_far(1, e, span, whole)
                if e == 0 and not exchanged:
                    exchange(0)
                    exchanged = True
                if d == chips - 1 and e == experts // 2:
                    forward(len(forwards))
    if not exchanged:
        exchange(0)
    for d in range(1, chips):
        span = arrive(1, chunks - 1, chunks, d)
        if d < chips - 1:
            for e in range(experts):
                add_far(1, e, span, whole)
    close(1, span)
    exchange(1)
    for b in range(2):
        at = band_of(b)
        pair_copy(b, chip).wait_recv()
        total = (part[chip * 2 + core, at, :].astype(jnp.float32)
                 + rxd[chip, at, :].astype(jnp.float32))
        for d in range(1, chips):
            sum_copy(b, d).wait_recv()
            total = total + rxx[d - 1, at, :].astype(jnp.float32)
        comb[at, :] = total.astype(jnp.bfloat16)

    for c in range(chunks):
        out_copy(c).wait()
        for b in range(2):
            side_copy(b, c).wait_send()
            for d in range(1, chips):
                cross_copy(b, c, d).wait_send()
                pass_copy(b, c, d).wait_send()
    for b in range(2):
        for j in range(chips):
            pair_copy(b, j).wait_send()
        for d in range(1, chips):
            sum_copy(b, d).wait_send()


def att_chunks(width):
    return width // (2 * HEAD_DIM)


def shards(dp_size, group, queries, key_states, value_states, doc_lengths, move_plan,
           expert_ids, gate_weights, expert_weight):
    rows, width = queries.shape
    experts, depth, ff = expert_weight.shape
    chips = group // 2
    chunks = att_chunks(width)
    owned = ff // group
    bf16, f32 = jnp.bfloat16, jnp.float32
    hbm = pl.BlockSpec(memory_space=pl.ANY)
    smem = pl.BlockSpec(memory_space=pltpu.SMEM)
    vmem = pl.BlockSpec(memory_space=pltpu.VMEM)
    dma = pltpu.SemaphoreType.DMA
    return pl.pallas_call(
        functools.partial(kernel, dp_size, group),
        out_shape=(
            jax.ShapeDtypeStruct((rows, width), bf16),
            jax.ShapeDtypeStruct((rows, owned), bf16),
            jax.ShapeDtypeStruct((1,), f32),
        ),
        in_specs=[hbm, hbm, hbm, smem, smem, vmem, vmem, hbm],
        out_specs=(hbm, vmem, smem),
        scratch_shapes=[
            pltpu.VMEM((rows, width), bf16),
            pltpu.VMEM((rows, width), bf16),
            pltpu.VMEM((rows, width), bf16),
            pltpu.VMEM((experts, depth, ff), bf16),
            pltpu.VMEM((rows, depth), bf16),
            pltpu.VMEM((experts, rows, ff), f32),
            pltpu.VMEM((rows, rows), f32),
            pltpu.VMEM((experts, rows, 128), f32),
            pltpu.VMEM((group, rows, owned), bf16),
            pltpu.VMEM((chips, rows, owned), bf16),
            pltpu.VMEM((chips - 1, rows, owned), bf16),
            pltpu.VMEM((chips - 1, rows, owned), bf16),
            dma((3, chunks)),
            dma((experts, chips, chunks, 2)),
            dma((chunks,)),
            dma((chips - 1, 2, chunks)),
            dma((chips - 1, 2, chunks)),
            dma((2, chunks)),
            dma((2, chunks)),
            dma((chips - 1, 2, chunks)),
            dma((chips - 1, 2, chunks)),
            dma((2, chips)),
            dma((2, chips)),
            dma((2, chips - 1)),
            dma((2, chips - 1)),
        ],
        compiler_params=pltpu.CompilerParams(
            collective_id=0, has_side_effects=True, vmem_limit_bytes=66_000_000),
    )(queries, key_states, value_states, doc_lengths, move_plan.T, expert_ids.T,
      gate_weights.T, expert_weight)


def solution(mesh):
    in_specs = (
        P("dp", "expert"),
        P("dp", "expert"),
        P("dp", "expert"),
        P(),
        P(),
        P("dp", None),
        P("dp", None),
        P("expert", None, None),
    )
    out_specs = (P("dp", "expert"), P("dp", "expert"), P("dp"))
    body = functools.partial(shards, mesh.shape["dp"], mesh.shape["expert"])
    return jax.shard_map(body, mesh=mesh, in_specs=in_specs, out_specs=out_specs, check_vma=False)
```

```python
import functools

import jax
import jax.numpy as jnp
from jax import lax
from jax.experimental import pallas as pl
from jax.experimental.pallas import tpu as pltpu
from jax.sharding import PartitionSpec as P

HEAD_DIM = 128
QBLOCK = 128
MESH = pl.DeviceIdType.MESH
LOG2E = 1.4426950408889634


def span_pairs(low, high, start, stop):
    first = jnp.maximum(low, start)
    last = jnp.minimum(high, stop)
    count = jnp.maximum(last - first, 0)
    return (count * ((first - start + 1) + (last - start))) // 2


def row_pairs(lens, row, block, docs, row_count):
    low = block * QBLOCK
    total = jnp.int32(0)
    picked = jnp.int32(0)
    edge = jnp.int32(0)
    for doc in range(docs):
        stop = edge + lens[row, doc]
        total = total + span_pairs(0, row_count, edge, stop)
        picked = picked + span_pairs(low, low + QBLOCK, edge, stop)
        edge = stop
    return total, picked


def kernel(dp_size, group, q_hbm, k_hbm, v_hbm, lens, plan, ids, gates, w_hbm,
           att_hbm, comb, load,
           qv, kv, vv, wv, xg, acc, bias, gsc, part, rxd, txx, rxx,
           in_sem, w_sem, out_sem,
           sx_sem, rx_sem, sd_sem, rd_sem, sf_sem, rf_sem,
           ps_sem, pr_sem, qs_sem, qr_sem):
    rows, width = q_hbm.shape
    experts, depth, ff = w_hbm.shape
    chips = group // 2
    ck = qv.shape[1] // att_chunks(width)
    chunks = width // ck
    chip_width = 2 * width
    step_width = 2 * ck
    owned = ff // group
    row = lax.axis_index("dp")
    me = lax.axis_index("expert")
    chip = me // 2
    core = lax.rem(me, 2)
    other = chip * 2 + 1 - core

    def in_copies(c):
        cols = pl.ds(pl.multiple_of(c * ck, 128), ck)
        return [
            pltpu.make_async_copy(src.at[:, cols], dst.at[:, cols], in_sem.at[i, c])
            for i, (src, dst) in enumerate(((q_hbm, qv), (k_hbm, kv), (v_hbm, vv)))
        ]

    def place(s, c, k):
        return pl.multiple_of(s * chip_width + c * step_width + k * ck, 128)

    def w_copy(e, s, c, k):
        src = pl.multiple_of((s * 2 + k) * width + c * ck, 128)
        return pltpu.make_async_copy(
            w_hbm.at[e, pl.ds(src, ck), :], wv.at[e, pl.ds(place(s, c, k), ck), :],
            w_sem.at[e, s, c, k])

    def w_start(e, s, c):
        for k in range(2):
            w_copy(e, s, c, k).start()

    def w_wait(e, s, c):
        for k in range(2):
            w_copy(e, s, c, k).wait()

    for c in range(chunks):
        for copy in in_copies(c):
            copy.start()

    barrier = pltpu.get_barrier_semaphore()
    pl.semaphore_signal(barrier, inc=1, device_id={"expert": other}, device_id_type=MESH)
    for d in range(1, chips):
        peer = lax.rem(chip + d, chips) * 2 + core
        pl.semaphore_signal(barrier, inc=1, device_id={"expert": peer}, device_id_type=MESH)

    def start_own(i, _):
        w_start(i // chunks, chip, lax.rem(i, chunks))
        return 0

    docs = lens.shape[1]
    column = lax.broadcasted_iota(jnp.int32, (rows, 1), 0)
    starts = jnp.zeros((rows, 1), jnp.int32)
    edge = jnp.int32(0)
    for doc in range(docs):
        edge = edge + lens[row, doc]
        starts = jnp.where(column >= edge, jnp.maximum(starts, edge), starts)

    pl.semaphore_wait(barrier, chips)

    half = rows // 2

    def band_of(b):
        return pl.ds(b * half, half)

    def cross_copy(b, c, d):
        at = xg.at[band_of(b), pl.ds(place(chip, c, core), ck)]
        return pltpu.make_async_remote_copy(
            src_ref=at, dst_ref=at,
            send_sem=sx_sem.at[d - 1, b, c], recv_sem=rx_sem.at[d - 1, b, c],
            device_id={"expert": lax.rem(chip + d, chips) * 2 + core}, device_id_type=MESH)

    def side_copy(b, c):
        at = xg.at[band_of(b), pl.ds(place(chip, c, core), ck)]
        return pltpu.make_async_remote_copy(
            src_ref=at, dst_ref=at,
            send_sem=sd_sem.at[b, c], recv_sem=rd_sem.at[b, c],
            device_id={"expert": other}, device_id_type=MESH)

    def pass_copy(b, c, d):
        at = xg.at[band_of(b), pl.ds(place(lax.rem(chip - d + chips, chips), c, core), ck)]
        return pltpu.make_async_remote_copy(
            src_ref=at, dst_ref=at,
            send_sem=sf_sem.at[d - 1, b, c], recv_sem=rf_sem.at[d - 1, b, c],
            device_id={"expert": other}, device_id_type=MESH)

    def out_copy(c):
        return pltpu.make_async_copy(
            xg.at[:, pl.ds(place(chip, c, core), ck)],
            att_hbm.at[:, pl.ds(pl.multiple_of(c * ck, 128), ck)], out_sem.at[c])

    scale = HEAD_DIM ** -0.5 * LOG2E

    for b in range(2):
        low, high = b * half, (b + 1) * half
        pos = lax.broadcasted_iota(jnp.int32, (half, high), 0) + low
        key_pos = lax.broadcasted_iota(jnp.int32, (half, high), 1)
        bias[low:high, :high] = jnp.where(
            (key_pos <= pos) & (key_pos >= starts[low:high]), 0.0, -1e30)

        def attend(c, _, b=b, low=low, high=high):
            if b == 0:
                for copy in in_copies(c):
                    copy.wait()
            for h in range(ck // HEAD_DIM):
                cols = pl.ds(pl.multiple_of(c * ck + h * HEAD_DIM, 128), HEAD_DIM)
                dst = pl.ds(pl.multiple_of(place(chip, c, core) + h * HEAD_DIM, 128), HEAD_DIM)
                s = lax.dot_general(
                    qv[low:high, cols], kv[:high, cols], (((1,), (1,)), ((), ())),
                    preferred_element_type=jnp.float32)
                s = s + bias[low:high, :high]
                top = jnp.max(s, axis=1, keepdims=True)
                p = jnp.exp2((s - top) * scale)
                norm = jnp.sum(p, axis=1, keepdims=True)
                o = jnp.dot(p.astype(jnp.bfloat16), vv[:high, cols],
                            preferred_element_type=jnp.float32)
                xg[low:high, dst] = (o / norm).astype(jnp.bfloat16)
            for d in range(1, chips):
                cross_copy(b, c, d).start()
            side_copy(b, c).start()
            if b == 1:
                out_copy(c).start()
            return 0

        lax.fori_loop(0, chunks, attend, 0)
        if b == 0:
            lax.fori_loop(0, experts * chunks, start_own, 0)

    for d in range(1, chips):
        def start_far(i, _, d=d):
            w_start(lax.rem(i, experts), lax.rem(chip - d + chips, chips), i // experts)
            return 0

        lax.fori_loop(0, experts * chunks, start_far, 0)

    partner = lax.rem(row + dp_size // 2, dp_size)
    own_total, own_moved = row_pairs(lens, row, plan[1, row], docs, rows)
    _, their_moved = row_pairs(lens, partner, plan[1, partner], docs, rows)
    work = own_total - jnp.where(plan[0, row] != row, own_moved, 0)
    work = work + jnp.where(plan[0, partner] != partner, their_moved, 0)
    load[0] = work.astype(jnp.float32) * (1.0 / (QBLOCK * QBLOCK))

    for e in range(experts):
        chosen = ids[...] == me * experts + e
        line = jnp.sum(jnp.where(chosen, gates[...], 0.0), axis=0, keepdims=True)
        for r in range(0, rows, 128):
            gsc[e, r:r + 128, :] = jnp.broadcast_to(line[:, r:r + 128], (128, 128)).T

    forwards = [(b, c, d) for b in range(2) for c in range(chunks) for d in range(1, chips)]
    per_half = len(forwards) // 2
    sent = [0]

    def forward(count):
        while sent[0] < min(count, len(forwards)):
            b, c, d = forwards[sent[0]]
            cross_copy(b, c, d).wait_recv()
            pass_copy(b, c, d).start()
            sent[0] += 1

    forward(1)
    for b in range(2):
        for c in range(chunks):
            side_copy(b, c).wait_recv()
    own = pl.ds(pl.multiple_of(chip * chip_width, 128), chip_width)
    tile = ff // 2
    for e in range(experts):
        def wait_own(c, _, e=e):
            w_wait(e, chip, c)
            return 0

        lax.fori_loop(0, chunks, wait_own, 0)

        def near(t, _, e=e):
            cols = pl.ds(pl.multiple_of(t * tile, 128), tile)
            acc[e, :, cols] = jnp.dot(xg[:, own], wv[e, own, cols],
                                      preferred_element_type=jnp.float32)
            return 0

        lax.fori_loop(0, 2, near, 0)
        forward(min(sent[0] + 1, per_half))

    def pair_copy(b, j):
        return pltpu.make_async_remote_copy(
            src_ref=part.at[j * 2 + 1 - core, band_of(b)], dst_ref=rxd.at[j, band_of(b)],
            send_sem=ps_sem.at[b, j], recv_sem=pr_sem.at[b, j],
            device_id={"expert": other}, device_id_type=MESH)

    def sum_copy(b, d):
        return pltpu.make_async_remote_copy(
            src_ref=txx.at[d - 1, band_of(b)], dst_ref=rxx.at[d - 1, band_of(b)],
            send_sem=qs_sem.at[b, d - 1], recv_sem=qr_sem.at[b, d - 1],
            device_id={"expert": lax.rem(chip + d, chips) * 2 + core}, device_id_type=MESH)

    def exchange(b):
        at = band_of(b)
        for d in range(1, chips):
            j = lax.rem(chip + d, chips)
            pair_copy(b, j).wait_recv()
            txx[d - 1, at, :] = (part[j * 2 + core, at, :].astype(jnp.float32)
                                 + rxd[j, at, :].astype(jnp.float32)).astype(jnp.bfloat16)
            sum_copy(b, d).start()

    def arrive(b, c0, c1, d):
        for c in range(c0, c1):
            forward(forwards.index((b, c, d)) + 1)
        for c in range(c0, c1):
            pass_copy(b, c, d).wait_recv()
            if b == 0:
                def wait_far(e, _, c=c, d=d):
                    w_wait(e, lax.rem(chip - d + chips, chips), c)
                    return 0

                lax.fori_loop(0, experts, wait_far, 0)
        return pl.ds(place(lax.rem(chip - d + chips, chips), c0, 0), (c1 - c0) * step_width)

    columns = 2 * owned
    rt = 64

    def add_far(b, e, span, cols):
        at = band_of(b)
        acc[e, at, cols] += jnp.dot(xg[at, span], wv[e, span, cols],
                                    preferred_element_type=jnp.float32)

    def close(b, span):
        for d in list(range(1, chips)) + [0]:
            j = lax.rem(chip + d, chips)
            cols = pl.ds(pl.multiple_of(j * columns, 128), columns)
            for e in range(experts):
                add_far(b, e, span, cols)

            def finish(r, _, cols=cols, j=j):
                at = pl.ds(pl.multiple_of(b * half + r * rt, rt), rt)
                total = jnp.zeros((rt, columns), jnp.float32)
                for e in range(experts):
                    h = acc[e, at, cols] * 0.5
                    total = total + (h * jnp.tanh(h) + h) * jnp.concatenate(
                        [gsc[e, at, :]] * (columns // 128), axis=1)
                total = total.astype(jnp.bfloat16)
                part[j * 2, at, :] = total[:, :owned]
                part[j * 2 + 1, at, :] = total[:, owned:]
                return 0

            lax.fori_loop(0, half // rt, finish, 0)
            pair_copy(b, j).start()

    whole = pl.ds(0, ff)
    for d in range(1, chips):
        span = arrive(0, 0, chunks, d)
        if d < chips - 1:
            for e in range(experts):
                add_far(0, e, span, whole)
    forward(per_half + 1)
    close(0, span)
    forward(per_half + 2)
    exchanged = False
    if chunks > 1:
        for d in range(1, chips):
            span = arrive(1, 0, chunks - 1, d)
            for e in range(experts):
                add_far(1, e, span, whole)
                if e == 0 and not exchanged:
                    exchange(0)
                    exchanged = True
                if d == chips - 1 and e == experts // 2:
                    forward(len(forwards))
    if not exchanged:
        exchange(0)
    for d in range(1, chips):
        span = arrive(1, chunks - 1, chunks, d)
        if d < chips - 1:
            for e in range(experts):
                add_far(1, e, span, whole)
    close(1, span)
    exchange(1)
    for b in range(2):
        at = band_of(b)
        pair_copy(b, chip).wait_recv()
        total = (part[chip * 2 + core, at, :].astype(jnp.float32)
                 + rxd[chip, at, :].astype(jnp.float32))
        for d in range(1, chips):
            sum_copy(b, d).wait_recv()
            total = total + rxx[d - 1, at, :].astype(jnp.float32)
        comb[at, :] = total.astype(jnp.bfloat16)

    for c in range(chunks):
        out_copy(c).wait()
        for b in range(2):
            side_copy(b, c).wait_send()
            for d in range(1, chips):
                cross_copy(b, c, d).wait_send()
                pass_copy(b, c, d).wait_send()
    for b in range(2):
        for j in range(chips):
            pair_copy(b, j).wait_send()
        for d in range(1, chips):
            sum_copy(b, d).wait_send()


def att_chunks(width):
    return width // (2 * HEAD_DIM)


def shards(dp_size, group, queries, key_states, value_states, doc_lengths, move_plan,
           expert_ids, gate_weights, expert_weight):
    rows, width = queries.shape
    experts, depth, ff = expert_weight.shape
    chips = group // 2
    chunks = att_chunks(width)
    owned = ff // group
    bf16, f32 = jnp.bfloat16, jnp.float32
    hbm = pl.BlockSpec(memory_space=pl.ANY)
    smem = pl.BlockSpec(memory_space=pltpu.SMEM)
    vmem = pl.BlockSpec(memory_space=pltpu.VMEM)
    dma = pltpu.SemaphoreType.DMA
    return pl.pallas_call(
        functools.partial(kernel, dp_size, group),
        out_shape=(
            jax.ShapeDtypeStruct((rows, width), bf16),
            jax.ShapeDtypeStruct((rows, owned), bf16),
            jax.ShapeDtypeStruct((1,), f32),
        ),
        in_specs=[hbm, hbm, hbm, smem, smem, vmem, vmem, hbm],
        out_specs=(hbm, vmem, smem),
        scratch_shapes=[
            pltpu.VMEM((rows, width), bf16),
            pltpu.VMEM((rows, width), bf16),
            pltpu.VMEM((rows, width), bf16),
            pltpu.VMEM((experts, depth, ff), bf16),
            pltpu.VMEM((rows, depth), bf16),
            pltpu.VMEM((experts, rows, ff), f32),
            pltpu.VMEM((rows, rows), f32),
            pltpu.VMEM((experts, rows, 128), f32),
            pltpu.VMEM((group, rows, owned), bf16),
            pltpu.VMEM((chips, rows, owned), bf16),
            pltpu.VMEM((chips - 1, rows, owned), bf16),
            pltpu.VMEM((chips - 1, rows, owned), bf16),
            dma((3, chunks)),
            dma((experts, chips, chunks, 2)),
            dma((chunks,)),
            dma((chips - 1, 2, chunks)),
            dma((chips - 1, 2, chunks)),
            dma((2, chunks)),
            dma((2, chunks)),
            dma((chips - 1, 2, chunks)),
            dma((chips - 1, 2, chunks)),
            dma((2, chips)),
            dma((2, chips)),
            dma((2, chips - 1)),
            dma((2, chips - 1)),
        ],
        compiler_params=pltpu.CompilerParams(
            collective_id=0, has_side_effects=True, vmem_limit_bytes=66_000_000),
    )(queries, key_states, value_states, doc_lengths, move_plan.T, expert_ids.T,
      gate_weights.T, expert_weight)


def solution(mesh):
    in_specs = (
        P("dp", "expert"),
        P("dp", "expert"),
        P("dp", "expert"),
        P(),
        P(),
        P("dp", None),
        P("dp", None),
        P("expert", None, None),
    )
    out_specs = (P("dp", "expert"), P("dp", "expert"), P("dp"))
    body = functools.partial(shards, mesh.shape["dp"], mesh.shape["expert"])
    return jax.shard_map(body, mesh=mesh, in_specs=in_specs, out_specs=out_specs, check_vma=False)
```
